32 devices in a mesh: shard: 8 (over z, y), tp: 4 (over x, core).
Axes of the slice: x: 2, y: 2, z: 4, core: 2. Of those that a mesh axis runs over, the one named last changes fastest.
Arguments:
- gradient: bfloat16 [4096, 16384], P('shard', 'tp'), may hold values from -2 to 2
- table: int32 [256, 3], replicated, may hold values from 0 to 31, as said below
- left_stat: bfloat16 [384, 512, 512], P(('shard', 'tp')), as said below
- right_stat: bfloat16 [384, 512, 512], P(('shard', 'tp')), as said below
- left_basis: bfloat16 [384, 512, 512], P(('shard', 'tp')), may hold values from -0.25 to 0.25
- right_basis: bfloat16 [384, 512, 512], P(('shard', 'tp')), may hold values from -0.25 to 0.25
- moment: bfloat16 [384, 512, 512], P(('shard', 'tp')), may hold values from -2 to 2
- second: float32 [384, 512, 512], P(('shard', 'tp')), may hold values from 0.02 to 0.2
Outputs:
- update: bfloat16 [4096, 16384], P('shard', 'tp')
- new_left: bfloat16 [384, 512, 512], P(('shard', 'tp'))
- new_right: bfloat16 [384, 512, 512], P(('shard', 'tp'))
- new_moment: bfloat16 [384, 512, 512], P(('shard', 'tp'))
- new_second: float32 [384, 512, 512], P(('shard', 'tp'))
The draws below stay inside these ranges and needn't reach their ends.
Inputs may be any that keep to these rules, and one draw needn't show every extreme that they name: `table`: column 0 is a block row below 8, column 1 a block column below 32, column 2 an owner device below 32; every block appears in exactly one row; each device owns between 4 and 12 blocks, and some device owns exactly 12. `left_stat`: Symmetric. `right_stat`: Symmetric.
All inputs are finite; a program needn't handle non-finite values.
Results may differ from the reference program's by a relative error of at most 0.0085.
Values may be sent and summed in bfloat16 or wider, within the bound.
A program may use at most 192 MiB of HBM per device.

```python
import math
import jax
import jax.numpy as jnp
from jax import lax

ROWS = 4096
COLS = 16384
BLOCK = 512
NDEV = 32
NBR = 8
NBC = 32
NBLK = 256
OWN_MEAN = 8
SLOTS = 12


def stat_draw(key, salt):
    key = jax.random.fold_in(key, salt)
    first_key, second_key = jax.random.split(key)
    count = NDEV * SLOTS
    diagonal = jax.random.uniform(first_key, (count, BLOCK), jnp.float32, 1.0, 2.0)
    noise = jax.random.normal(second_key, (count, BLOCK, BLOCK), jnp.float32)
    symmetric = (noise + jnp.swapaxes(noise, 1, 2)) * (0.25 / jnp.sqrt(jnp.float32(BLOCK)))
    return symmetric + jnp.eye(BLOCK, dtype=jnp.float32)[None, :, :] * diagonal[:, None, :]


def draw_left_stat(key, part):
    return stat_draw(key, 11).astype(jnp.bfloat16)


def draw_right_stat(key, part):
    return stat_draw(key, 23).astype(jnp.bfloat16)


def draw_table(key, part):
    keys = jax.random.split(key, 4)
    reach = (OWN_MEAN + 1) // 2
    halfway = NDEV // 2
    shifts = jax.random.randint(keys[0], (halfway,), 0, reach + 1)
    shifts = shifts.at[0].set(reach)
    counts = jnp.concatenate([OWN_MEAN + shifts, OWN_MEAN - shifts])
    counts = counts[jax.random.permutation(keys[1], NDEV)]
    bounds = jnp.cumsum(counts)
    places = jnp.arange(NBLK, dtype=jnp.int32)
    owner_of = jnp.sum((bounds[None, :] <= places[:, None]).astype(jnp.int32), axis=1)
    blocks = jax.random.permutation(keys[2], NBLK).astype(jnp.int32)
    order = jax.random.permutation(keys[3], NBLK)
    owners = owner_of[order]
    return jnp.stack([blocks // NBC, blocks % NBC, owners], axis=1).astype(jnp.int32)


def level_of(key, extent, shards, low, top_value):
    level = 1.0
    for position, parts in shards:
        heights = jax.random.uniform(jax.random.fold_in(jax.random.fold_in(key, 6), position), (parts,), jnp.float32, low / len(shards), top_value / len(shards))
        level = level * jnp.repeat(jnp.exp(heights), extent[position] // parts).reshape((-1,) + (1,) * (len(extent) - 1 - position))
    return level


def gaussian(own_key, extent, width, bound, cuts=(), kind=jnp.bfloat16):
    level = level_of(own_key, extent, cuts, -0.22, 0.18) if cuts else 1.0
    array = jax.random.normal(own_key, extent, jnp.float32) * width * level
    return jnp.minimum(jnp.maximum(array, -bound), bound).astype(kind)


def setup_inputs(seed: int = 0) -> dict:
    arg_keys = jax.random.split(jax.random.key(seed), 9)
    return {
        "gradient": gaussian(arg_keys[0], (ROWS, COLS), 0.25, 2.0, ((0, 8), (1, 4))),
        "table": draw_table(jax.random.fold_in(arg_keys[8], 71), 0),
        "left_stat": draw_left_stat(jax.random.fold_in(arg_keys[8], 71), 0),
        "right_stat": draw_right_stat(jax.random.fold_in(arg_keys[8], 71), 0),
        "left_basis": gaussian(arg_keys[4], (NDEV * SLOTS, BLOCK, BLOCK), BLOCK ** -0.5, 0.25, ((0, 32),)),
        "right_basis": gaussian(arg_keys[5], (NDEV * SLOTS, BLOCK, BLOCK), BLOCK ** -0.5, 0.25, ((0, 32),)),
        "moment": gaussian(arg_keys[6], (NDEV * SLOTS, BLOCK, BLOCK), 0.25, 2.0, ((0, 32),)),
        "second": jnp.clip(jnp.exp(math.log(0.2) - 2.3025851 * jax.random.uniform(arg_keys[7], (NDEV * SLOTS, BLOCK, BLOCK), jnp.float32) ** level_of(arg_keys[7], (NDEV * SLOTS, BLOCK, BLOCK), ((0, 32),), -0.2, 0.2)), 0.02, 0.2),
    }


beta_moment = 0.9
beta_second = 0.95
beta_stats = 0.95
epsilon = 1e-08

def slot_table(table, slots):
    owners = table[:, 2]
    count = owners.shape[0]
    order = jnp.arange(count, dtype=jnp.int32)
    earlier = (owners[None, :] == owners[:, None]) & (order[None, :] < order[:, None])
    slot_rank = lax.optimization_barrier(jnp.sum(earlier.astype(jnp.int32), axis=1)).astype(jnp.int32)
    return (owners * slots + slot_rank).astype(jnp.int32)

def precondition(grad_block, left, right, left_q, right_q, first, squares):
    left_new = (beta_stats * left.astype(jnp.float32) + (1.0 - beta_stats) * jnp.dot(grad_block, grad_block.T, preferred_element_type=jnp.float32)).astype(jnp.bfloat16)
    right_new = (beta_stats * right.astype(jnp.float32) + (1.0 - beta_stats) * jnp.dot(grad_block.T, grad_block, preferred_element_type=jnp.float32)).astype(jnp.bfloat16)
    first_new = (beta_moment * first.astype(jnp.float32) + (1.0 - beta_moment) * grad_block.astype(jnp.float32)).astype(jnp.bfloat16)
    left_grad = jnp.dot(left_q.T, grad_block, preferred_element_type=jnp.float32).astype(jnp.bfloat16)
    rotated = jnp.dot(left_grad, right_q, preferred_element_type=jnp.float32)
    squares_new = beta_second * squares + (1.0 - beta_second) * rotated * rotated
    left_first = jnp.dot(left_q.T, first_new, preferred_element_type=jnp.float32).astype(jnp.bfloat16)
    first_rot = jnp.dot(left_first, right_q, preferred_element_type=jnp.float32)
    scaled = (first_rot / (jnp.sqrt(squares_new) + epsilon)).astype(jnp.bfloat16)
    back = jnp.dot(left_q, scaled, preferred_element_type=jnp.float32).astype(jnp.bfloat16)
    result = jnp.dot(back, right_q.T, preferred_element_type=jnp.float32).astype(jnp.bfloat16)
    return (result, left_new, right_new, first_new, squares_new)

def reference(gradient, table, left_stat, right_stat, left_basis, right_basis, moment, second):
    tiles = gradient.reshape(NBR, BLOCK, NBC, BLOCK).transpose(0, 2, 1, 3).reshape(NBLK, BLOCK, BLOCK)
    state_row = slot_table(table, SLOTS)
    block_id = (table[:, 0] * NBC + table[:, 1]).astype(jnp.int32)

    def one_block(index):
        slot = state_row[index]
        return precondition(tiles[block_id[index]], left_stat[slot], right_stat[slot], left_basis[slot], right_basis[slot], moment[slot], second[slot])
    results = lax.map(one_block, jnp.arange(NBLK, dtype=jnp.int32))
    block_updates, left_rows, right_rows, first_rows, square_rows = results
    new_left = left_stat.at[state_row].set(left_rows)
    new_right = right_stat.at[state_row].set(right_rows)
    new_moment = moment.at[state_row].set(first_rows)
    new_second = second.at[state_row].set(square_rows)
    placed = jnp.zeros((NBLK, BLOCK, BLOCK), jnp.bfloat16).at[block_id].set(block_updates)
    update = placed.reshape(NBR, NBC, BLOCK, BLOCK).transpose(0, 2, 1, 3).reshape(ROWS, COLS)
    return (update, new_left, new_right, new_moment, new_second)
```

```python
import functools

import jax
import jax.numpy as jnp
from jax import lax
from jax.experimental import pallas as pl
from jax.experimental.pallas import tpu as pltpu
from jax.sharding import PartitionSpec as P

beta_moment = 0.9
beta_second = 0.95
beta_stats = 0.95
epsilon = 1e-08
AXES = ("shard", "tp")


def slot_table(table, slots):
    owners = table[:, 2]
    count = owners.shape[0]
    order = jnp.arange(count, dtype=jnp.int32)
    earlier = (owners[None, :] == owners[:, None]) & (order[None, :] < order[:, None])
    slot_rank = jnp.sum(earlier.astype(jnp.int32), axis=1)
    return owners * slots + slot_rank


def exchange(array):
    return lax.all_to_all(array, AXES, split_axis=0, concat_axis=0, tiled=True)


def dot(a, b, dims):
    return lax.dot_general(a, b, (dims, ((), ())), preferred_element_type=jnp.float32)


def pack_kernel(group, slots, first, count, halves, tp_count, side, src_ref, col_ref, in_ref, out_ref):
    base = pl.program_id(0) * group

    def device(d, carry):
        for k in range(count):
            entry = (base + d) * slots + first + k
            src = src_ref[entry]
            col = pl.multiple_of(col_ref[entry] * side, side)
            for h in range(halves):
                out_ref[d, k, h] = in_ref[src + h * tp_count, :, pl.ds(col, side)]
        return carry

    lax.fori_loop(0, group, device, 0)


def pack(received, src, col, slots, first, count, halves, tp_count, side):
    dev_count, rows, cols = received.shape
    group = 4 if dev_count % 4 == 0 else 1
    return pl.pallas_call(
        functools.partial(pack_kernel, group, slots, first, count, halves, tp_count, side),
        grid_spec=pltpu.PrefetchScalarGridSpec(
            num_scalar_prefetch=2,
            grid=(dev_count // group,),
            in_specs=[pl.BlockSpec((dev_count, rows, cols), lambda i, *_: (0, 0, 0))],
            out_specs=pl.BlockSpec((group, count, halves, rows, side), lambda i, *_: (i, 0, 0, 0, 0)),
        ),
        out_shape=jax.ShapeDtypeStruct((dev_count, count, halves, rows, side), received.dtype),
        cost_estimate=pl.CostEstimate(flops=0, bytes_accessed=received.size * 6, transcendentals=0),
    )(src, col, received)


def unpack_kernel(group, firsts, halves, tp_count, cols_per_dev, side, own_ref, slot_ref, *refs):
    out_ref = refs[-1]
    base = pl.program_id(0) * group

    def device(d, carry):
        dev = base + d
        shard = dev // tp_count
        half = shard % halves
        place = (shard // halves * tp_count + dev % tp_count) * cols_per_dev
        for c in range(cols_per_dev):
            owner = own_ref[place + c]
            slot = slot_ref[place + c]
            value = refs[0][owner, jnp.minimum(slot, refs[0].shape[1] - 1), half]
            for ref, first in zip(refs[1:-1], firsts[1:]):
                inner = jnp.clip(slot - first, 0, ref.shape[1] - 1)
                value = jnp.where(slot >= first, ref[owner, inner, half], value)
            out_ref[d, :, c * side : (c + 1) * side] = value
        return carry

    lax.fori_loop(0, group, device, 0)


def unpack(chunks, firsts, own, slot, tp_count, cols_per_dev):
    dev_count, _, halves, rows, side = chunks[0].shape
    group = 4 if dev_count % 4 == 0 else 1
    cols = cols_per_dev * side
    return pl.pallas_call(
        functools.partial(unpack_kernel, group, firsts, halves, tp_count, cols_per_dev, side),
        grid_spec=pltpu.PrefetchScalarGridSpec(
            num_scalar_prefetch=2,
            grid=(dev_count // group,),
            in_specs=[pl.BlockSpec(c.shape, lambda i, *_: (0, 0, 0, 0, 0)) for c in chunks],
            out_specs=pl.BlockSpec((group, rows, cols), lambda i, *_: (i, 0, 0)),
        ),
        out_shape=jax.ShapeDtypeStruct((dev_count, rows, cols), chunks[0].dtype),
        cost_estimate=pl.CostEstimate(flops=0, bytes_accessed=dev_count * rows * cols * 5, transcendentals=0),
    )(own, slot, *chunks)


def slot_kernel(first, packed, mine_ref, x_ref, left, right, left_q, right_q, moment, second, *refs):
    out_ref, left_o, right_o, moment_o, second_o = refs[-5:]
    side = left.shape[-1]
    used = mine_ref[first + pl.program_id(0)] > 0

    @pl.when(used)
    def _():
        if packed:
            halves = x_ref.shape[2]
            parts = [x_ref[:, 0, h].reshape(side // halves, side) for h in range(halves)]
            grad = parts[0] if halves == 1 else jnp.concatenate(parts, axis=0)
        else:
            grad = x_ref[0]
        ql = left_q[0]
        qr = right_q[0]
        first_new = (
            beta_moment * moment[0].astype(jnp.float32)
            + (1.0 - beta_moment) * grad.astype(jnp.float32)
        ).astype(jnp.bfloat16)
        moment_o[0] = first_new
        left_grad = dot(ql, grad, ((0,), (0,))).astype(jnp.bfloat16)
        rotated = dot(left_grad, qr, ((1,), (0,)))
        squares_new = beta_second * second[0] + (1.0 - beta_second) * rotated * rotated
        second_o[0] = squares_new
        left_first = dot(ql, first_new, ((0,), (0,))).astype(jnp.bfloat16)
        first_rot = dot(left_first, qr, ((1,), (0,)))
        scaled = (first_rot / (jnp.sqrt(squares_new) + epsilon)).astype(jnp.bfloat16)
        back = dot(ql, scaled, ((1,), (0,))).astype(jnp.bfloat16)
        result = dot(back, qr, ((1,), (1,))).astype(jnp.bfloat16)
        if packed:
            halves = x_ref.shape[2]
            step = side // halves
            for h in range(halves):
                out_ref[:, 0, h] = result[h * step : (h + 1) * step].reshape(
                    x_ref.shape[0], x_ref.shape[3], side
                )
        else:
            out_ref[0] = result
        left_o[0] = (
            beta_stats * left[0].astype(jnp.float32)
            + (1.0 - beta_stats) * dot(grad, grad, ((1,), (1,)))
        ).astype(jnp.bfloat16)
        right_o[0] = (
            beta_stats * right[0].astype(jnp.float32)
            + (1.0 - beta_stats) * dot(grad, grad, ((0,), (0,)))
        ).astype(jnp.bfloat16)

    @pl.when(jnp.logical_not(used))
    def _():
        out_ref[...] = jnp.zeros_like(out_ref)
        left_o[...] = left[...]
        right_o[...] = right[...]
        moment_o[...] = moment[...]
        second_o[...] = second[...]


def precondition(x, mine, states, done, first, packed):
    left = states[0]
    slots, side, _ = left.shape
    if packed:
        dev_count, count, halves, rows, _ = x.shape
        x_spec = pl.BlockSpec((dev_count, 1, halves, rows, side), lambda i, *_: (0, i, 0, 0, 0))
    else:
        count = x.shape[0]
        x_spec = pl.BlockSpec((1, side, side), lambda i, *_: (i, 0, 0))
    state_spec = pl.BlockSpec((1, side, side), lambda i, *_: (first + i, 0, 0))
    done = list(done)
    kept = [jax.ShapeDtypeStruct(states[k].shape, states[k].dtype) for k in (0, 1, 4, 5)]
    return pl.pallas_call(
        functools.partial(slot_kernel, first, packed),
        grid_spec=pltpu.PrefetchScalarGridSpec(
            num_scalar_prefetch=1,
            grid=(count,),
            in_specs=[x_spec] + [state_spec] * 6 + [pl.BlockSpec(memory_space=pl.ANY)] * len(done),
            out_specs=[x_spec] + [state_spec] * 4,
        ),
        out_shape=[jax.ShapeDtypeStruct(x.shape, x.dtype)] + kept,
        input_output_aliases={8 + k: 1 + k for k in range(len(done))},
        cost_estimate=pl.CostEstimate(
            flops=count * 16 * side**3,
            bytes_accessed=count * side * side * 26,
            transcendentals=count * side * side,
        ),
    )(mine, x, *states, *done)


CAPS = (19, 21, 23, 26)
MESH = pl.DeviceIdType.MESH


class Route:
    def __init__(self, shard_count, tp_count, slots, side, cols_per_dev, cap, spare):
        self.near = 2
        self.tp_count = tp_count
        self.planes = shard_count // self.near
        self.wing = self.planes // 2
        self.group = self.near * tp_count
        self.slots = slots
        self.side = side
        self.cols = cols_per_dev
        self.stripe = side // self.group
        self.rows = 16
        self.chunks = self.stripe // self.rows
        self.held = self.group * cols_per_dev
        self.cap = min(cap, self.held)
        self.near_cap = min(cap + spare, self.held)

    def me(self):
        shard = lax.axis_index("shard")
        return shard // self.near, (shard % self.near) * self.tp_count + lax.axis_index("tp")

    def device(self, plane, member):
        return (plane * self.near + member // self.tp_count, member % self.tp_count)

    def hops(self):
        out = [(1, e, self.cap) for e in range(self.wing)]
        return out + [(0, e, self.near_cap) for e in range(1, self.wing)]

    def plane_at(self, plane, cross, step):
        wing, place = plane // self.wing, plane % self.wing
        if cross:
            wing = 1 - wing
        return wing * self.wing + (place + step) % self.wing

    def plane_from(self, plane, cross, step):
        return self.plane_at(plane, cross, self.wing - step)


def usable(shard_count, tp_count, row_dev, side):
    group = 2 * tp_count
    return row_dev == side and shard_count % 4 == 0 and side % (16 * group) == 0


def greet(route):
    plane, member = route.me()
    barrier = pltpu.get_barrier_semaphore()
    count = 0
    for i in range(1, route.group):
        peer = route.device(plane, (member + i) % route.group)
        pl.semaphore_signal(barrier, inc=1, device_id=peer, device_id_type=MESH)
        count += 1
    for cross, step, _ in route.hops():
        peer = route.device(route.plane_at(plane, cross, step), member)
        pl.semaphore_signal(barrier, inc=1, device_id=peer, device_id_type=MESH)
        count += 1
    pl.semaphore_wait(barrier, count)


class Spread:
    def __init__(self, route, src_of, dst_of, whole, sems, h, pieces):
        send, recv = sems
        plane, member = route.me()
        self.parts, self.own, self.waits = [], [], []

        def remote(src, dst, i):
            return pltpu.make_async_remote_copy(
                src_ref=src,
                dst_ref=dst,
                send_sem=send.at[h, i],
                recv_sem=recv.at[h, i],
                device_id=route.device(plane, (member + i) % route.group),
                device_id_type=MESH,
            )

        for i in range(1, route.group):
            other = (member + i) % route.group
            self.parts += [remote(src_of(other, c), dst_of(member, c), i) for c in range(pieces)]
            self.waits.append(remote(whole, whole, i))
        self.own = [
            pltpu.make_async_copy(src_of(member, c), dst_of(member, c), recv.at[h, 0])
            for c in range(pieces)
        ]
        self.own_wait = pltpu.make_async_copy(whole, whole, recv.at[h, 0])

    def start(self):
        start_all(self.parts + self.own)

    def wait_recv(self):
        for copy in self.waits:
            copy.wait_recv()
        self.own_wait.wait()

    def wait_send(self):
        for copy in self.waits:
            copy.wait_send()


def to_planes(route, src, dst, sems, h):
    send, recv = sems
    plane, member = route.me()
    copies = []
    for n, (cross, step, cap) in enumerate(route.hops()):
        other = route.plane_at(plane, cross, step)
        copies.append(
            pltpu.make_async_remote_copy(
                src_ref=src.at[other, pl.ds(0, cap)],
                dst_ref=dst.at[plane, pl.ds(0, cap)],
                send_sem=send.at[h, n],
                recv_sem=recv.at[h, n],
                device_id=route.device(other, member),
                device_id_type=MESH,
            )
        )
    return copies


def fill_planes(route, load, out, kept):
    plane, _ = route.me()

    def fill(ref, at, cap):
        def one(k, carry):
            ref[at, k] = load(at * route.held + k)
            return carry

        lax.fori_loop(0, cap, one, 0)

    for cross, step, cap in route.hops():
        fill(out, route.plane_at(plane, cross, step), cap)
    fill(kept, plane, route.near_cap)


def start_all(copies):
    for copy in copies:
        copy.start()


def recv_all(copies):
    for copy in copies:
        copy.wait_recv()


def pipeline(route, enter, turn, leave):
    for h in range(route.chunks):
        enter(h)
    for h in range(route.chunks + 1):
        if h < route.chunks:
            turn(h)
        if h >= 1:
            leave(h - 1)


def split_scratch(route, refs):
    n = route.chunks
    return [refs[i * n : (i + 1) * n] for i in range(4)], [refs[4 * n + 2 * i : 4 * n + 2 * i + 2] for i in range(3)]


def columns(ref, m, h, c, side):
    return ref.at[m, h, :, pl.ds(c * side, side)]


def forward_kernel(route, zj_ref, zc_ref, dp_ref, dk_ref, g_ref, x_ref, *refs):
    (tile, outz, inz, outd), (sem_a, sem_z, sem_d) = split_scratch(route, refs)
    greet(route)
    stage = {}

    def enter(h):
        stage["a", h] = Spread(
            route,
            lambda m, c: columns(g_ref, m, h, c, route.side),
            lambda m, c: tile[h].at[m, c],
            tile[h].at[0],
            sem_a,
            h,
            route.cols,
        )
        stage["a", h].start()

    def turn(h):
        stage["a", h].wait_recv()

        def load(at):
            return tile[h][zj_ref[at], zc_ref[at]]

        fill_planes(route, load, outz[h], inz[h])
        stage["z", h] = to_planes(route, outz[h], inz[h], sem_z, h)
        start_all(stage["z", h])

    def leave(h):
        recv_all(stage["z", h])

        def member(m, carry):
            for s in range(route.slots):
                at = m * route.slots + s
                outd[h][m, s] = inz[h][dp_ref[at], dk_ref[at]]
            return carry

        lax.fori_loop(0, route.group, member, 0)
        stage["d", h] = Spread(
            route,
            lambda m, c: outd[h].at[m],
            lambda m, c: x_ref.at[:, m, h],
            outd[h].at[0],
            sem_d,
            h,
            1,
        )
        stage["d", h].start()

    pipeline(route, enter, turn, leave)
    finish(route, stage, "d")


def finish(route, stage, last):
    for h in range(route.chunks):
        stage[last, h].wait_recv()
    for h in range(route.chunks):
        stage["a", h].wait_send()
        for copy in stage["z", h]:
            copy.wait_send()
        stage["d", h].wait_send()


def backward_kernel(route, zj_ref, zs_ref, fp_ref, fk_ref, u_ref, g_ref, *refs):
    (tile, outz, inz, ind), (sem_a, sem_z, sem_d) = split_scratch(route, refs)
    greet(route)
    stage = {}

    def enter(h):
        stage["d", h] = Spread(
            route,
            lambda m, c: u_ref.at[:, m, h],
            lambda m, c: ind[h].at[m],
            ind[h].at[0],
            sem_d,
            h,
            1,
        )
        stage["d", h].start()

    def turn(h):
        stage["d", h].wait_recv()

        def load(at):
            return ind[h][zj_ref[at], zs_ref[at]]

        fill_planes(route, load, outz[h], inz[h])
        stage["z", h] = to_planes(route, outz[h], inz[h], sem_z, h)
        start_all(stage["z", h])

    def leave(h):
        recv_all(stage["z", h])

        def member(m, carry):
            for c in range(route.cols):
                at = m * route.cols + c
                tile[h][m, c] = inz[h][fp_ref[at], fk_ref[at]]
            return carry

        lax.fori_loop(0, route.group, member, 0)
        stage["a", h] = Spread(
            route,
            lambda m, c: tile[h].at[m, c],
            lambda m, c: columns(g_ref, m, h, c, route.side),
            tile[h].at[0],
            sem_a,
            h,
            route.cols,
        )
        stage["a", h].start()

    pipeline(route, enter, turn, leave)
    finish(route, stage, "a")


def travel(kernel, route, collective_id, lists, data, out_shape):
    dtype = data.dtype
    piece = (route.rows, route.side)
    tile = pltpu.VMEM((route.group, route.cols) + piece, dtype)
    lanes = pltpu.VMEM((route.planes, route.near_cap) + piece, dtype)
    slots = pltpu.VMEM((route.group, route.slots) + piece, dtype)
    sems = [pltpu.SemaphoreType.DMA((route.chunks, n)) for n in (route.group, route.planes, route.group) for _ in range(2)]
    moved = data.size * data.dtype.itemsize
    return pl.pallas_call(
        functools.partial(kernel, route),
        in_specs=[pl.BlockSpec(memory_space=pltpu.SMEM)] * len(lists) + [pl.BlockSpec(memory_space=pl.ANY)],
        out_specs=pl.BlockSpec(memory_space=pl.ANY),
        out_shape=jax.ShapeDtypeStruct(out_shape, dtype),
        scratch_shapes=[s for s in (tile, lanes, lanes, slots) for _ in range(route.chunks)] + sems,
        compiler_params=pltpu.CompilerParams(
            collective_id=collective_id, has_side_effects=True, vmem_limit_bytes=60 * 1024 * 1024
        ),
        cost_estimate=pl.CostEstimate(flops=moved * 400, bytes_accessed=moved * 4, transcendentals=0),
    )(*lists, data)


def pick(keys, count, *values):
    hit = keys[None, :] == jnp.arange(count, dtype=jnp.int32)[:, None]
    return [jnp.sum(jnp.where(hit, v[None, :], 0), axis=1) for v in values]


def routed(gradient, table, states):
    shard_count, tp_count = lax.axis_size("shard"), lax.axis_size("tp")
    slots, side, _ = states[0].shape
    row_dev, col_dev = gradient.shape
    cols = col_dev // side

    def make(cap):
        return Route(shard_count, tp_count, slots, side, cols, cap, 4)

    base = make(1)
    held, group, planes = base.held, base.group, base.planes
    rows, count = table.shape[0], planes * held
    owner = table[:, 2]
    src = table[:, 0] * tp_count + table[:, 1] // cols
    a, j, c = src // group, src % group, table[:, 1] % cols
    b, m = owner // group, owner % group
    pair = a * planes + b
    order = jnp.arange(rows, dtype=jnp.int32)
    earlier = order[None, :] < order[:, None]
    s = jnp.sum((earlier & (owner[None, :] == owner[:, None])).astype(jnp.int32), axis=1)
    k = jnp.sum((earlier & (pair[None, :] == pair[:, None])).astype(jnp.int32), axis=1)
    crosses = (a // base.wing) != (b // base.wing)
    most = jnp.max(jnp.where(crosses, k + 1, k + 1 - 4))
    which = jnp.sum((most > jnp.array(CAPS, dtype=jnp.int32)).astype(jnp.int32))

    plane, member = base.me()
    out_key = jnp.where(a == plane, b * held + k, -1)
    zj, zc = pick(out_key, count, j, c)
    own_key = jnp.where(b == plane, m * slots + s, -1)
    dp, dk = pick(own_key, group * slots, a, k)
    back_key = jnp.where(b == plane, a * held + k, -1)
    rj, rs = pick(back_key, count, m, s)
    home_key = jnp.where(a == plane, j * cols + c, -1)
    fp, fk = pick(home_key, held, b, k)
    myself = plane * group + member
    mine = pick(jnp.where(owner == myself, s, -1), slots, jnp.ones_like(s))[0]

    routes = [make(cap) for cap in CAPS + (held,)]
    piece = (base.chunks, base.rows)
    block_shape = (slots, group) + piece + (side,)
    grad_shape = (group,) + piece + (col_dev,)

    def forward(i):
        return lambda g: travel(forward_kernel, routes[i], 2 * i, (zj, zc, dp, dk), g, block_shape)

    def backward(i):
        return lambda u: travel(backward_kernel, routes[i], 2 * i + 1, (rj, rs, fp, fk), u, grad_shape)

    everyone = range(len(routes))
    x = lax.switch(which, [forward(i) for i in everyone], gradient.reshape(grad_shape))
    x = x.reshape(slots, side, side)
    update, *done = precondition(x, mine, states, (), 0, False)
    update = lax.switch(which, [backward(i) for i in everyone], update.reshape(block_shape))
    return (update.reshape(row_dev, col_dev), *done)


def shards(gradient, table, left_stat, right_stat, left_basis, right_basis, moment, second):
    shard_count = lax.axis_size("shard")
    tp_count = lax.axis_size("tp")
    dev_count = shard_count * tp_count
    row_dev, col_dev = gradient.shape
    slots = left_stat.shape[0]
    side = left_stat.shape[1]
    if usable(shard_count, tp_count, row_dev, side):
        states = (left_stat, right_stat, left_basis, right_basis, moment, second)
        return routed(gradient, table, states)
    halves = side // row_dev
    cols_per_dev = col_dev // side
    block_cols = tp_count * cols_per_dev
    rows = row_dev // dev_count
    packed = rows % 16 == 0
    received = exchange(gradient.reshape(dev_count, rows, col_dev))

    state_row = slot_table(table, slots)
    block_id = table[:, 0] * block_cols + table[:, 1]
    targets = jnp.arange(dev_count * slots, dtype=jnp.int32)
    matches = (state_row[None, :] == targets[:, None]).astype(jnp.int32)
    send_id = jnp.sum(matches * block_id[None, :], axis=1)
    filled = jnp.sum(matches, axis=1)
    send_col = send_id % block_cols
    src = (send_id // block_cols) * halves * tp_count + send_col // cols_per_dev
    col = send_col % cols_per_dev
    myself = lax.axis_index(AXES)
    mine = lax.dynamic_slice_in_dim(filled, myself * slots, slots)
    positions = jnp.arange(table.shape[0], dtype=jnp.int32)
    block_match = (block_id[None, :] == positions[:, None]).astype(jnp.int32)
    slot_of_block = jnp.sum(block_match * state_row[None, :], axis=1)
    own = slot_of_block // slots
    slot = slot_of_block % slots

    half = (slots + 1) // 2
    chunks = [(0, half), (half, slots - half)] if slots > 1 else [(0, slots)]
    states = (left_stat, right_stat, left_basis, right_basis, moment, second)
    tiles = received.reshape(dev_count, rows, cols_per_dev, side)
    half_index = jnp.arange(halves, dtype=jnp.int32)
    inbox = []
    for first, count in chunks:
        if packed:
            out = pack(received, src, col, slots, first, count, halves, tp_count, side)
        else:
            src_c = src.reshape(dev_count, slots)[:, first : first + count]
            col_c = col.reshape(dev_count, slots)[:, first : first + count]
            out = tiles[src_c[:, :, None] + half_index * tp_count, :, col_c[:, :, None]]
        inbox.append(exchange(out))
    done = ()
    returned = []
    for x, (first, count) in zip(inbox, chunks):
        if not packed:
            x = x.transpose(1, 2, 0, 3, 4).reshape(count, side, side)
        update, *done = precondition(x, mine, states, done, first, packed)
        if not packed:
            update = update.reshape(count, halves, dev_count, rows, side).transpose(2, 0, 1, 3, 4)
        returned.append(exchange(update))
    if packed:
        outbox = unpack(returned, tuple(f for f, _ in chunks), own, slot, tp_count, cols_per_dev)
    else:
        back = jnp.concatenate(returned, axis=1)
        dev = jnp.arange(dev_count, dtype=jnp.int32)[:, None]
        place = (dev // tp_count // halves * tp_count + dev % tp_count) * cols_per_dev
        place = place + jnp.arange(cols_per_dev, dtype=jnp.int32)[None, :]
        picked = back[own[place], slot[place], dev // tp_count % halves]
        outbox = picked.transpose(0, 2, 1, 3).reshape(dev_count, rows, col_dev)
    update = exchange(outbox).reshape(row_dev, col_dev)
    new_left, new_right, new_moment, new_second = done
    return (update, new_left, new_right, new_moment, new_second)


def solution(mesh):
    state = P(AXES, None, None)
    in_specs = (P("shard", "tp"), P()) + (state,) * 6
    out_specs = (P("shard", "tp"),) + (state,) * 4
    return jax.shard_map(shards, mesh=mesh, in_specs=in_specs, out_specs=out_specs, check_vma=False)
```

```python
import functools
import math

import jax
import jax.numpy as jnp
from jax import lax
from jax.experimental import pallas as pl
from jax.experimental.pallas import tpu as pltpu
from jax.sharding import PartitionSpec as P

beta_moment = 0.9
beta_second = 0.95
beta_stats = 0.95
epsilon = 1e-08
AXES = ("shard", "tp")


def slot_table(table, slots):
    owners = table[:, 2]
    count = owners.shape[0]
    order = jnp.arange(count, dtype=jnp.int32)
    earlier = (owners[None, :] == owners[:, None]) & (order[None, :] < order[:, None])
    slot_rank = jnp.sum(earlier.astype(jnp.int32), axis=1)
    return owners * slots + slot_rank


def exchange(array):
    return lax.all_to_all(array, AXES, split_axis=0, concat_axis=0, tiled=True)


def dot(a, b, dims):
    return lax.dot_general(a, b, (dims, ((), ())), preferred_element_type=jnp.float32)


def pack_kernel(group, slots, first, count, halves, tp_count, side, src_ref, col_ref, in_ref, out_ref):
    base = pl.program_id(0) * group

    def device(d, carry):
        for k in range(count):
            entry = (base + d) * slots + first + k
            src = src_ref[entry]
            col = pl.multiple_of(col_ref[entry] * side, side)
            for h in range(halves):
                out_ref[d, k, h] = in_ref[src + h * tp_count, :, pl.ds(col, side)]
        return carry

    lax.fori_loop(0, group, device, 0)


def pack(received, src, col, slots, first, count, halves, tp_count, side):
    dev_count, rows, cols = received.shape
    group = 4 if dev_count % 4 == 0 else 1
    return pl.pallas_call(
        functools.partial(pack_kernel, group, slots, first, count, halves, tp_count, side),
        grid_spec=pltpu.PrefetchScalarGridSpec(
            num_scalar_prefetch=2,
            grid=(dev_count // group,),
            in_specs=[pl.BlockSpec((dev_count, rows, cols), lambda i, *_: (0, 0, 0))],
            out_specs=pl.BlockSpec((group, count, halves, rows, side), lambda i, *_: (i, 0, 0, 0, 0)),
        ),
        out_shape=jax.ShapeDtypeStruct((dev_count, count, halves, rows, side), received.dtype),
        cost_estimate=pl.CostEstimate(flops=0, bytes_accessed=received.size * 6, transcendentals=0),
    )(src, col, received)


def unpack_kernel(group, firsts, halves, tp_count, cols_per_dev, side, own_ref, slot_ref, *refs):
    out_ref = refs[-1]
    base = pl.program_id(0) * group

    def device(d, carry):
        dev = base + d
        shard = dev // tp_count
        half = shard % halves
        place = (shard // halves * tp_count + dev % tp_count) * cols_per_dev
        for c in range(cols_per_dev):
            owner = own_ref[place + c]
            slot = slot_ref[place + c]
            value = refs[0][owner, jnp.minimum(slot, refs[0].shape[1] - 1), half]
            for ref, first in zip(refs[1:-1], firsts[1:]):
                inner = jnp.clip(slot - first, 0, ref.shape[1] - 1)
                value = jnp.where(slot >= first, ref[owner, inner, half], value)
            out_ref[d, :, c * side : (c + 1) * side] = value
        return carry

    lax.fori_loop(0, group, device, 0)


def unpack(chunks, firsts, own, slot, tp_count, cols_per_dev):
    dev_count, _, halves, rows, side = chunks[0].shape
    group = 4 if dev_count % 4 == 0 else 1
    cols = cols_per_dev * side
    return pl.pallas_call(
        functools.partial(unpack_kernel, group, firsts, halves, tp_count, cols_per_dev, side),
        grid_spec=pltpu.PrefetchScalarGridSpec(
            num_scalar_prefetch=2,
            grid=(dev_count // group,),
            in_specs=[pl.BlockSpec(c.shape, lambda i, *_: (0, 0, 0, 0, 0)) for c in chunks],
            out_specs=pl.BlockSpec((group, rows, cols), lambda i, *_: (i, 0, 0)),
        ),
        out_shape=jax.ShapeDtypeStruct((dev_count, rows, cols), chunks[0].dtype),
        cost_estimate=pl.CostEstimate(flops=0, bytes_accessed=dev_count * rows * cols * 5, transcendentals=0),
    )(own, slot, *chunks)


def slot_kernel(first, packed, mine_ref, x_ref, left, right, left_q, right_q, moment, second, *refs):
    out_ref, left_o, right_o, moment_o, second_o = refs[-5:]
    side = left.shape[-1]
    used = mine_ref[first + pl.program_id(0)] > 0

    @pl.when(used)
    def _():
        if packed:
            halves = x_ref.shape[2]
            parts = [x_ref[:, 0, h].reshape(side // halves, side) for h in range(halves)]
            grad = parts[0] if halves == 1 else jnp.concatenate(parts, axis=0)
        else:
            grad = x_ref[0]
        ql = left_q[0]
        qr = right_q[0]
        first_new = (
            beta_moment * moment[0].astype(jnp.float32)
            + (1.0 - beta_moment) * grad.astype(jnp.float32)
        ).astype(jnp.bfloat16)
        moment_o[0] = first_new
        left_grad = dot(ql, grad, ((0,), (0,))).astype(jnp.bfloat16)
        rotated = dot(left_grad, qr, ((1,), (0,)))
        squares_new = beta_second * second[0] + (1.0 - beta_second) * rotated * rotated
        second_o[0] = squares_new
        left_first = dot(ql, first_new, ((0,), (0,))).astype(jnp.bfloat16)
        first_rot = dot(left_first, qr, ((1,), (0,)))
        scaled = (first_rot / (jnp.sqrt(squares_new) + epsilon)).astype(jnp.bfloat16)
        back = dot(ql, scaled, ((1,), (0,))).astype(jnp.bfloat16)
        result = dot(back, qr, ((1,), (1,))).astype(jnp.bfloat16)
        if packed:
            halves = x_ref.shape[2]
            step = side // halves
            for h in range(halves):
                out_ref[:, 0, h] = result[h * step : (h + 1) * step].reshape(
                    x_ref.shape[0], x_ref.shape[3], side
                )
        else:
            out_ref[0] = result
        left_o[0] = (
            beta_stats * left[0].astype(jnp.float32)
            + (1.0 - beta_stats) * dot(grad, grad, ((1,), (1,)))
        ).astype(jnp.bfloat16)
        right_o[0] = (
            beta_stats * right[0].astype(jnp.float32)
            + (1.0 - beta_stats) * dot(grad, grad, ((0,), (0,)))
        ).astype(jnp.bfloat16)

    @pl.when(jnp.logical_not(used))
    def _():
        out_ref[...] = jnp.zeros_like(out_ref)
        left_o[...] = left[...]
        right_o[...] = right[...]
        moment_o[...] = moment[...]
        second_o[...] = second[...]


def precondition(x, mine, states, done, first, packed):
    left = states[0]
    slots, side, _ = left.shape
    if packed:
        dev_count, count, halves, rows, _ = x.shape
        x_spec = pl.BlockSpec((dev_count, 1, halves, rows, side), lambda i, *_: (0, i, 0, 0, 0))
    else:
        count = x.shape[0]
        x_spec = pl.BlockSpec((1, side, side), lambda i, *_: (i, 0, 0))
    state_spec = pl.BlockSpec((1, side, side), lambda i, *_: (first + i, 0, 0))
    done = list(done)
    kept = [jax.ShapeDtypeStruct(states[k].shape, states[k].dtype) for k in (0, 1, 4, 5)]
    return pl.pallas_call(
        functools.partial(slot_kernel, first, packed),
        grid_spec=pltpu.PrefetchScalarGridSpec(
            num_scalar_prefetch=1,
            grid=(count,),
            in_specs=[x_spec] + [state_spec] * 6 + [pl.BlockSpec(memory_space=pl.ANY)] * len(done),
            out_specs=[x_spec] + [state_spec] * 4,
        ),
        out_shape=[jax.ShapeDtypeStruct(x.shape, x.dtype)] + kept,
        input_output_aliases={8 + k: 1 + k for k in range(len(done))},
        cost_estimate=pl.CostEstimate(
            flops=count * 16 * side**3,
            bytes_accessed=count * side * side * 26,
            transcendentals=count * side * side,
        ),
    )(mine, x, *states, *done)


MARGINS = (1, 2, 3, 5, 8)
SPARE = 8
SPILL = 6
MESH = pl.DeviceIdType.MESH


class Route:
    def __init__(self, shard_count, tp_count, slots, side, cols_per_dev, cap):
        self.near = 2
        self.tp_count = tp_count
        self.planes = shard_count // self.near
        self.wing = self.planes // 2
        self.group = self.near * tp_count
        self.slots = slots
        self.side = side
        self.cols = cols_per_dev
        self.rows = 8
        self.chunks = side // self.group // self.rows
        self.held = self.group * cols_per_dev
        self.cap = min(cap, self.held)
        self.near_cap = min(cap + SPARE, self.held)
        self.spill = min(SPILL, slots, cols_per_dev)

    def me(self):
        shard = lax.axis_index("shard")
        return shard // self.near, (shard % self.near) * self.tp_count + lax.axis_index("tp")

    def device(self, plane, member):
        return (plane * self.near + member // self.tp_count, member % self.tp_count)

    def hops(self):
        return [(1, 0, self.cap), (1, 1, self.cap), (0, 1, self.near_cap)]

    def plane_at(self, plane, cross, step):
        wing, place = plane // self.wing, plane % self.wing
        if cross:
            wing = 1 - wing
        return wing * self.wing + (place + step) % self.wing


def usable(shard_count, tp_count, row_dev, side):
    return row_dev == side and shard_count == 8 and side % (16 * tp_count) == 0


def greet(route):
    plane, member = route.me()
    barrier = pltpu.get_barrier_semaphore()
    count = 0
    for i in range(1, route.group):
        peer = route.device(plane, (member + i) % route.group)
        pl.semaphore_signal(barrier, inc=1, device_id=peer, device_id_type=MESH)
        count += 1
    for cross, step, _ in route.hops():
        peer = route.device(route.plane_at(plane, cross, step), member)
        pl.semaphore_signal(barrier, inc=1, device_id=peer, device_id_type=MESH)
        count += 1
    pl.semaphore_wait(barrier, count)


class Spread:
    def __init__(self, route, peers, src_of, dst_of, whole, sems, h, pieces):
        self.route, self.peers, self.src_of, self.dst_of, self.whole = route, peers, src_of, dst_of, whole
        self.send, self.recv = sems
        self.h, self.pieces = h, pieces

    def remote(self, src, dst, i):
        return pltpu.make_async_remote_copy(
            src_ref=src,
            dst_ref=dst,
            send_sem=self.send.at[self.h, i],
            recv_sem=self.recv.at[self.h, i],
            device_id=self.peers[i][1],
            device_id_type=MESH,
        )

    def start(self):
        member = self.peers[0][0]

        def piece(c):
            for i in range(1, self.route.group):
                self.remote(self.src_of(self.peers[i][0], c), self.dst_of(member, c), i).start()
            pltpu.make_async_copy(
                self.src_of(member, c), self.dst_of(member, c), self.recv.at[self.h, 0]
            ).start()

        repeat(self.pieces, piece)

    def wait_recv(self):
        for i in range(1, self.route.group):
            self.remote(self.whole, self.whole, i).wait_recv()
        pltpu.make_async_copy(self.whole, self.whole, self.recv.at[self.h, 0]).wait()

    def wait_send(self):
        for i in range(1, self.route.group):
            self.remote(self.whole, self.whole, i).wait_send()


class Planes:
    def __init__(self, route, src, dst, sems, h):
        send, recv = sems
        plane, member = route.me()
        self.copies = []
        for n, (cross, step, cap) in enumerate(route.hops()):
            other = route.plane_at(plane, cross, step)
            self.copies.append(
                pltpu.make_async_remote_copy(
                    src_ref=src.at[other, pl.ds(0, cap)],
                    dst_ref=dst.at[plane, pl.ds(0, cap)],
                    send_sem=send.at[h, n],
                    recv_sem=recv.at[h, n],
                    device_id=route.device(other, member),
                    device_id_type=MESH,
                )
            )

    def start(self):
        for copy in self.copies:
            copy.start()

    def wait_recv(self):
        for copy in self.copies:
            copy.wait_recv()

    def wait_send(self):
        for copy in self.copies:
            copy.wait_send()


def detour(route, src, dst, sems, h):
    send, recv = sems
    plane, member = route.me()
    return pltpu.make_async_remote_copy(
        src_ref=src,
        dst_ref=dst,
        send_sem=send.at[h, 0],
        recv_sem=recv.at[h, 0],
        device_id=route.device(route.plane_at(plane, 0, 1), member),
        device_id_type=MESH,
    )


def repeat(count, body):
    def one(i, carry):
        body(i)
        return carry

    lax.fori_loop(0, count, one, 0)


def fill_planes(route, load, out, kept):
    plane, _ = route.me()

    def fill(ref, at, cap):
        def one(k):
            ref[at, k] = load(at * route.held + k)

        repeat(cap, one)

    for cross, step, cap in route.hops():
        fill(out, route.plane_at(plane, cross, step), cap)
    fill(kept, plane, route.near_cap)


def run_stages(route, enter, swap, turn, leave):
    chunks = route.chunks
    started = [0, 0, 0]

    def upto(n, stage, end):
        while started[n] < min(end, chunks):
            stage(started[n])
            started[n] += 1

    upto(0, enter, 2)
    upto(1, swap, 1)
    upto(0, enter, 4)
    upto(1, swap, 2)
    upto(2, turn, 2)
    for t in range(chunks):
        upto(0, enter, t + 6)
        upto(1, swap, t + 4)
        upto(2, turn, t + 2)
        leave(t)


def split_scratch(route, refs):
    n = route.chunks
    return [refs[i * n : (i + 1) * n] for i in range(6)], [refs[6 * n + 2 * i : 6 * n + 2 * i + 2] for i in range(4)]


def columns(ref, m, h, c, side):
    return ref.at[m, h, :, pl.ds(pl.multiple_of(c * side, side), side)]


def exchange_kernel(route, inward, list_ref, in_ref, out_ref, *refs):
    (gathered, outz, inz, outs, outy, iny), (sem_a, sem_z, sem_d, sem_y) = split_scratch(route, refs)
    early, lane, final = (0, 2, 4) if inward else (6, 8, 10)
    greet(route)
    plane, member = route.me()
    others = [(member + i) % route.group for i in range(route.group)]
    peers = [(other, route.device(plane, other)) for other in others]
    chunks = range(route.chunks)
    count = route.slots if inward else route.cols
    step = math.gcd(count, 4)

    def parts(hbm, buf, h, by_column, sems, leaving):
        if by_column:
            far, near, pieces = lambda m, c: columns(hbm, m, h, c, route.side), lambda m, c: buf.at[m, c], route.cols
        else:
            far, near, pieces = lambda m, c: hbm.at[:, m, h], lambda m, c: buf.at[m], 1
        ends = (near, far) if leaving else (far, near)
        return Spread(route, peers, *ends, buf.at[0], sems, h, pieces)

    spread = [parts(in_ref, gathered[h], h, inward, sem_a, False) for h in chunks]
    extra = [detour(route, outy[h], iny[h], sem_y, h) for h in chunks]
    cross = [Planes(route, outz[h], inz[h], sem_z, h) for h in chunks]
    deliver = [parts(out_ref, outs[h], h, not inward, sem_d, True) for h in chunks]

    def swap(h):
        spread[h].wait_recv()

        def one(v):
            outy[h][v] = gathered[h][list_ref[early, v], list_ref[early + 1, v]]

        repeat(route.spill, one)
        extra[h].start()

    def turn(h):
        extra[h].wait_recv()

        def late(v):
            gathered[h][route.group, v] = iny[h][v]

        repeat(route.spill, late)
        fill_planes(route, lambda at: gathered[h][list_ref[lane, at], list_ref[lane + 1, at]], outz[h], inz[h])
        cross[h].start()

    def leave(h):
        cross[h].wait_recv()

        def member(m):
            def several(first):
                for i in range(step):
                    n = first * step + i
                    at = m * count + n
                    outs[h][m, n] = inz[h][list_ref[final, at], list_ref[final + 1, at]]

            repeat(count // step, several)

        repeat(route.group, member)
        deliver[h].start()

    run_stages(route, lambda h: spread[h].start(), swap, turn, leave)
    for h in chunks:
        deliver[h].wait_recv()
    for copies in spread + extra + cross + deliver:
        copies.wait_send()


def travel(route, inward, collective_id, lists, data, out_shape):
    dtype = data.dtype
    piece = (route.rows, route.side)
    counts = (route.cols, route.slots) if inward else (route.slots, route.cols)
    gathered = pltpu.VMEM((route.group + 1, counts[0]) + piece, dtype)
    lanes = pltpu.VMEM((route.planes, route.near_cap) + piece, dtype)
    outs = pltpu.VMEM((route.group, counts[1]) + piece, dtype)
    late = pltpu.VMEM((route.spill,) + piece, dtype)
    sems = [pltpu.SemaphoreType.DMA((route.chunks, n)) for n in (route.group, route.planes, route.group, 1) for _ in range(2)]
    moved = data.size * data.dtype.itemsize
    return pl.pallas_call(
        functools.partial(exchange_kernel, route, inward),
        in_specs=[pl.BlockSpec(memory_space=pltpu.SMEM), pl.BlockSpec(memory_space=pl.ANY)],
        out_specs=pl.BlockSpec(memory_space=pl.ANY),
        out_shape=jax.ShapeDtypeStruct(out_shape, dtype),
        scratch_shapes=[s for s in (gathered, lanes, lanes, outs, late, late) for _ in range(route.chunks)] + sems,
        compiler_params=pltpu.CompilerParams(
            collective_id=collective_id, has_side_effects=True, vmem_limit_bytes=60 * 1024 * 1024
        ),
        cost_estimate=pl.CostEstimate(flops=moved * 400, bytes_accessed=moved * 4, transcendentals=0),
    )(lists, data)


FIELDS = ("a", "j", "c", "wing_a", "twin_a", "b", "m", "wing_b", "twin_b", "owner")
WHICH = 12
MINE = 14


def plan_kernel(base, caps, row_ref, col_ref, out_ref):
    planes, held, width, blocks = base.planes, base.held, out_ref.shape[1], row_ref.shape[1]

    class Side:
        pass

    row, col = Side(), Side()
    for i, name in enumerate(FIELDS):
        setattr(row, name, row_ref[i : i + 1, :])
        setattr(col, name, col_ref[:, i : i + 1])
    row.n = lax.broadcasted_iota(jnp.int32, (1, blocks), 1).astype(jnp.float32)
    col.n = lax.broadcasted_iota(jnp.int32, (blocks, 1), 0).astype(jnp.float32)
    lanes = lax.broadcasted_iota(jnp.int32, (1, width), 1).astype(jnp.float32)
    plane, member = base.me()
    me = (plane * base.group + member).astype(jnp.float32)
    plane = plane.astype(jnp.float32)

    def one(mask):
        return jnp.where(mask, 1.0, 0.0)

    def tally(name, weight):
        setattr(row, name, jnp.sum(weight(row, col), axis=0, keepdims=True))
        setattr(col, name, jnp.sum(weight(col, row), axis=1, keepdims=True))

    def pick(key, value):
        return jnp.sum(jnp.where(key == lanes, value, 0.0), axis=0, keepdims=True)

    def put(at, value):
        out_ref[at : at + 1, :] = jnp.broadcast_to(value, (1, width)).astype(jnp.int32)

    tally("s", lambda n, x: one(x.n < n.n) * one(x.owner == n.owner))
    tally("q", lambda n, x: one(x.n < n.n) * one(x.a == n.a) * one(x.b == n.b))
    tally("pair", lambda n, x: one(x.a == n.a) * one(x.b == n.b))
    for side in (row, col):
        side.cross = one(side.wing_a != side.wing_b)
    put(MINE, pick(jnp.where(col.owner == me, col.s, -1.0), 1.0))

    def way(at, p0, t0, x0, i0, p1, x1, i1, size1):
        def get(side, name):
            return getattr(side, name)

        tally("twins", lambda n, x: one(get(x, p0) == get(n, t0)) * one(get(x, p1) == get(n, p1)))
        half = row.pair + row.twins
        need = jnp.max(jnp.where(row.cross > 0, half * 0.5, row.pair - SPARE), axis=1, keepdims=True)
        cap, which = jnp.full((1, 1), caps[0], jnp.float32), jnp.zeros((1, 1), jnp.float32)
        for this, larger in zip(caps[:-1], caps[1:]):
            over = row.cross * one(row.q >= this)
            spilled = jnp.zeros((1, 1), jnp.float32)
            for p in range(planes):
                spilled = jnp.maximum(spilled, jnp.sum(over * one(get(row, p0) == p), axis=1, keepdims=True))
            small = jnp.maximum(one(need > this), one(spilled > base.spill))
            cap, which = cap + small * (larger - this), which + small
        put(WHICH + at, which)
        for side in (row, col):
            side.moved = side.cross * one(side.q >= cap)
        tally("v", lambda n, x: one(x.n < n.n) * x.moved * one(get(x, p0) == get(n, p0)))
        moved = col.moved > 0
        launch = jnp.where(moved, get(col, t0), get(col, p0))
        k = jnp.where(moved, col.twins + col.q - cap, col.q)
        early = jnp.where(get(col, p0) == plane, jnp.where(moved, col.v, -1.0), -1.0)
        lane = jnp.where(launch == plane, get(col, p1) * held + k, -1.0)
        final = jnp.where(get(col, p1) == plane, get(col, x1) * size1 + get(col, i1), -1.0)
        values = (
            (early, get(col, x0)),
            (early, get(col, i0)),
            (lane, jnp.where(moved, float(base.group), get(col, x0))),
            (lane, jnp.where(moved, col.v, get(col, i0))),
            (final, launch),
            (final, k),
        )
        for i, (key, value) in enumerate(values):
            put(6 * at + i, pick(key, value))

    way(0, "a", "twin_a", "j", "c", "b", "m", "s", base.slots)
    way(1, "b", "twin_b", "m", "s", "a", "j", "c", base.cols)


def make_plan(base, caps, table, tp_count):
    group, wing = base.group, base.wing
    owner = table[:, 2]
    src = table[:, 0] * tp_count + table[:, 1] // base.cols
    a, b = src // group, owner // group
    fields = [a, src % group, table[:, 1] % base.cols, a // wing, a // wing * wing + (a % wing + 1) % wing]
    fields += [b, owner % group, b // wing, b // wing * wing + (b % wing + 1) % wing, owner]
    columns_of = jnp.stack(fields, axis=1).astype(jnp.float32)
    return pl.pallas_call(
        functools.partial(plan_kernel, base, caps),
        out_shape=jax.ShapeDtypeStruct((16, base.planes * base.held), jnp.int32),
        cost_estimate=pl.CostEstimate(flops=10**7, bytes_accessed=10**5, transcendentals=0),
    )(columns_of.T, columns_of)


def routed(gradient, table, states):
    shard_count, tp_count = lax.axis_size("shard"), lax.axis_size("tp")
    slots, side, _ = states[0].shape
    row_dev, col_dev = gradient.shape
    cols = col_dev // side

    def make(cap):
        return Route(shard_count, tp_count, slots, side, cols, cap)

    base = make(1)
    held = base.held
    caps = tuple(held // base.planes + extra for extra in MARGINS) + (held,)
    routes = [make(cap) for cap in caps]
    plan = make_plan(base, caps, table, tp_count)
    mine = plan[MINE, :slots]
    piece = (base.chunks, base.rows)
    block_shape = (slots, base.group) + piece + (side,)
    grad_shape = (base.group,) + piece + (col_dev,)

    def move(data, inward, shape):
        def branch(n):
            return lambda d: travel(routes[n], inward, 2 * n + int(inward), plan, d, shape)

        which = plan[WHICH + int(not inward), 0]
        return lax.switch(which, [branch(n) for n in range(len(routes))], data)

    x = move(gradient.reshape(grad_shape), True, block_shape)
    update, *done = precondition(x.reshape(slots, side, side), mine, states, (), 0, False)
    update = move(update.reshape(block_shape), False, grad_shape)
    return (update.reshape(row_dev, col_dev), *done)


def shards(gradient, table, left_stat, right_stat, left_basis, right_basis, moment, second):
    shard_count = lax.axis_size("shard")
    tp_count = lax.axis_size("tp")
    dev_count = shard_count * tp_count
    row_dev, col_dev = gradient.shape
    slots = left_stat.shape[0]
    side = left_stat.shape[1]
    if usable(shard_count, tp_count, row_dev, side):
        states = (left_stat, right_stat, left_basis, right_basis, moment, second)
        return routed(gradient, table, states)
    halves = side // row_dev
    cols_per_dev = col_dev // side
    block_cols = tp_count * cols_per_dev
    rows = row_dev // dev_count
    packed = rows % 16 == 0
    received = exchange(gradient.reshape(dev_count, rows, col_dev))

    state_row = slot_table(table, slots)
    block_id = table[:, 0] * block_cols + table[:, 1]
    targets = jnp.arange(dev_count * slots, dtype=jnp.int32)
    matches = (state_row[None, :] == targets[:, None]).astype(jnp.int32)
    send_id = jnp.sum(matches * block_id[None, :], axis=1)
    filled = jnp.sum(matches, axis=1)
    send_col = send_id % block_cols
    src = (send_id // block_cols) * halves * tp_count + send_col // cols_per_dev
    col = send_col % cols_per_dev
    myself = lax.axis_index(AXES)
    mine = lax.dynamic_slice_in_dim(filled, myself * slots, slots)
    positions = jnp.arange(table.shape[0], dtype=jnp.int32)
    block_match = (block_id[None, :] == positions[:, None]).astype(jnp.int32)
    slot_of_block = jnp.sum(block_match * state_row[None, :], axis=1)
    own = slot_of_block // slots
    slot = slot_of_block % slots

    half = (slots + 1) // 2
    chunks = [(0, half), (half, slots - half)] if slots > 1 else [(0, slots)]
    states = (left_stat, right_stat, left_basis, right_basis, moment, second)
    tiles = received.reshape(dev_count, rows, cols_per_dev, side)
    half_index = jnp.arange(halves, dtype=jnp.int32)
    inbox = []
    for first, count in chunks:
        if packed:
            out = pack(received, src, col, slots, first, count, halves, tp_count, side)
        else:
            src_c = src.reshape(dev_count, slots)[:, first : first + count]
            col_c = col.reshape(dev_count, slots)[:, first : first + count]
            out = tiles[src_c[:, :, None] + half_index * tp_count, :, col_c[:, :, None]]
        inbox.append(exchange(out))
    done = ()
    returned = []
    for x, (first, count) in zip(inbox, chunks):
        if not packed:
            x = x.transpose(1, 2, 0, 3, 4).reshape(count, side, side)
        update, *done = precondition(x, mine, states, done, first, packed)
        if not packed:
            update = update.reshape(count, halves, dev_count, rows, side).transpose(2, 0, 1, 3, 4)
        returned.append(exchange(update))
    if packed:
        outbox = unpack(returned, tuple(f for f, _ in chunks), own, slot, tp_count, cols_per_dev)
    else:
        back = jnp.concatenate(returned, axis=1)
        dev = jnp.arange(dev_count, dtype=jnp.int32)[:, None]
        place = (dev // tp_count // halves * tp_count + dev % tp_count) * cols_per_dev
        place = place + jnp.arange(cols_per_dev, dtype=jnp.int32)[None, :]
        picked = back[own[place], slot[place], dev // tp_count % halves]
        outbox = picked.transpose(0, 2, 1, 3).reshape(dev_count, rows, col_dev)
    update = exchange(outbox).reshape(row_dev, col_dev)
    new_left, new_right, new_moment, new_second = done
    return (update, new_left, new_right, new_moment, new_second)


def solution(mesh):
    state = P(AXES, None, None)
    in_specs = (P("shard", "tp"), P()) + (state,) * 6
    out_specs = (P("shard", "tp"),) + (state,) * 4
    return jax.shard_map(shards, mesh=mesh, in_specs=in_specs, out_specs=out_specs, check_vma=False)
```
